32 devices in a mesh: ops: 8 (over z, core), blk: 4 (over y, x).
Axes of the slice: x: 2, y: 2, z: 4, core: 2. Of those that a mesh axis runs over, the one named last changes fastest.
Arguments:
- psi: bfloat16 [2048, 1024], P('blk'), may hold values from -6 to 6
- left_blocks: bfloat16 [64, 16, 128, 128], P('ops', 'blk'), may hold values from -0.5 to 0.5
- right_ops: bfloat16 [64, 1024, 1024], P(('ops', 'blk')), may hold values from -0.046875 to 0.046875
- block_target: int32 [64, 16], P('ops'), may hold values from 0 to 15
- left_partner: int32 [64], P('ops'), may hold values from 0 to 63, as said below
- block_len: int32 [16], replicated, may hold values from 1 to 128, 1536 in all
Outputs:
- sigma: bfloat16 [2048, 1024], P('blk', 'ops')
The draws below stay inside these ranges and needn't reach their ends.
Inputs may be any that keep to these rules, and one draw needn't show every extreme that they name: left_partner is a permutation of 0 to 63 that maps each aligned group of 8 operators onto itself.
All inputs are finite; a program needn't handle non-finite values.
Results may differ from the reference program's by a relative error of at most 0.018.
Values may be sent and summed in bfloat16 or wider, within the bound.
A program may use at most 128 MiB of HBM per device.

```python
import math
import jax
import jax.numpy as jnp
import numpy as np
from jax import lax

BOND = 2048
BS = 128
RW = 1024
NB = 16
K = 64
OPS_GROUP = 8


def draw_left_partner(key, part):
    scores = jax.random.randint(key, (K,), 0, 65536, dtype=jnp.int32) * K + jnp.arange(K, dtype=jnp.int32)
    groups = K // OPS_GROUP
    order = jnp.argsort(scores.reshape(groups, OPS_GROUP), axis=1, stable=True).astype(jnp.int32)
    shifted = order + jnp.arange(groups, dtype=jnp.int32)[:, None] * OPS_GROUP
    return shifted.reshape(K).astype(jnp.int32)


def with_ends(values, stream_key, low, top_value):
    extent = values.shape
    place = [jax.random.randint(jax.random.fold_in(stream_key, axis), (), 0, extent[axis]) for axis in range(len(extent))]
    values = values.at[tuple(place)].set(low)
    longest = extent.index(max(extent))
    place[longest] = (place[longest] + 1) % extent[longest]
    return values.at[tuple(place)].set(top_value)


def with_spikes(array, rng, source, target, parts, factor):
    owner, partner = [(jnp.arange(array.shape[axis_at]) // (array.shape[axis_at] // parts)).reshape([-1 if axis == axis_at else 1 for axis in range(array.ndim)]) for axis_at in (source, target)]
    chosen = jax.random.permutation(rng, parts)[partner]
    strong = (owner == chosen) | (owner == (partner + parts // 2) % parts)
    return jnp.where(strong, factor * array, array)


def level_of(key, extent, split, smallest, top_value):
    factor_of = 1.0
    for position, parts in split:
        draws = jax.random.uniform(jax.random.fold_in(jax.random.fold_in(key, 6), position), (parts,), jnp.float32, smallest / len(split), top_value / len(split))
        factor_of = factor_of * jnp.repeat(jnp.exp(draws), extent[position] // parts).reshape((-1,) + (1,) * (len(extent) - 1 - position))
    return factor_of


def profile(count, total, reach, skew):
    weights = [(1 << 20) // math.isqrt(rank ** skew) + 1 for rank in range(2, count + 1)]
    surplus, holding = total - reach - (count - 1), [1] * (count - 1)
    while surplus > 0:
        candidates = [i for i in range(count - 1) if holding[i] < reach]
        mass, remaining = sum([weights[i] for i in candidates]), surplus
        for i in candidates:
            more = min(reach - holding[i], max(1, remaining * weights[i] // mass), surplus)
            holding[i] = holding[i] + more
            surplus = surplus - more
    return np.array([reach] + holding)


def uneven_parts(stream_key, amount, total, bound, skew):
    if amount == 2:
        one = jax.random.randint(stream_key, (), max(1, total - bound), min(bound, total - 1) + 1)
        return jnp.stack([one, total - one])
    lengths = jnp.asarray(profile(amount, total, bound, skew), jnp.int32)
    couples = (amount - 1) // 2
    source_of, taker = lengths[1:1 + 2 * couples:2], lengths[2:2 + 2 * couples:2]
    room = jnp.minimum(source_of - 1, bound - taker)
    moved = jax.random.randint(jax.random.fold_in(stream_key, 1), (couples,), 0, 1 << 20) % (room + 1)
    lengths = lengths.at[1:1 + 2 * couples:2].set(source_of - moved).at[2:2 + 2 * couples:2].set(taker + moved)
    return lengths[jax.random.permutation(jax.random.fold_in(stream_key, 2), amount)]


def noise(own_key, extent, scale, reach, shards=(), held_as=jnp.bfloat16):
    gain = level_of(own_key, extent, shards, -0.22, 0.18) if shards else 1.0
    values = jax.random.normal(own_key, extent, jnp.float32) * scale * gain
    return jnp.minimum(jnp.maximum(values, -reach), reach).astype(held_as)


def gaussian_with(own_key, shape, spread, limit, shards, heavy, kind=jnp.bfloat16):
    drawn = spread * jax.random.normal(own_key, shape, jnp.float32)
    if shards:
        drawn = drawn * level_of(own_key, shape, shards, -0.22, 0.18)
    return jnp.clip(with_spikes(drawn, jax.random.fold_in(own_key, 3), *heavy), -limit, limit).astype(kind)


def setup_inputs(seed: int = 0) -> dict:
    streams_of = jax.random.split(jax.random.key(seed), 7)
    psi = noise(streams_of[0], (BOND, RW), 1.0, 6.0, ((0, 4),))
    left_blocks = noise(streams_of[1], (K, NB, BS, BS), BS ** -0.5, 0.5, ((0, 8), (1, 4)))
    right_ops = gaussian_with(streams_of[2], (K, RW, RW), (RW * K) ** -0.5, 0.046875, ((0, 32),), (0, 2, 32, 2.75))
    block_target = with_ends(jax.random.randint(streams_of[3], (K, NB), 0, NB), jax.random.fold_in(streams_of[3], 1), 0, NB - 1).astype(jnp.int32)
    left_partner = draw_left_partner(jax.random.fold_in(streams_of[6], 71), 0)
    block_len = uneven_parts(streams_of[5], NB, 3 * BOND // 4, BS, 2).astype(jnp.int32)
    return dict(psi=psi, left_blocks=left_blocks, right_ops=right_ops, block_target=block_target, left_partner=left_partner, block_len=block_len)


def reference(psi, left_blocks, right_ops, block_target, left_partner, block_len):
    nblocks = BOND // BS
    row_index = jnp.arange(BS, dtype=jnp.int32)
    live_rows = row_index[None, :] < block_len[:, None]
    masked = psi.reshape(nblocks, BS, RW) * live_rows[:, :, None].astype(jnp.bfloat16)
    states = masked.reshape(BOND, RW).astype(jnp.float32)

    def absorb(totals, index):
        image = jnp.dot(states, right_ops[index].astype(jnp.float32), precision=lax.Precision.HIGHEST)
        image = lax.optimization_barrier(image.astype(jnp.bfloat16)).astype(jnp.float32)
        image = image.reshape(nblocks, BS, RW)
        owner = left_partner[index]
        mixed = jnp.einsum("qab,qbr->qar", left_blocks[owner].astype(jnp.float32), image, precision=lax.Precision.HIGHEST)
        totals = totals + jax.ops.segment_sum(mixed, block_target[owner], num_segments=nblocks)
        return totals, None

    start = jnp.zeros((nblocks, BS, RW), jnp.float32)
    totals = lax.scan(absorb, start, jnp.arange(K, dtype=jnp.int32))[0]
    result = totals * live_rows[:, :, None].astype(jnp.float32)
    return result.reshape(BOND, RW).astype(jnp.bfloat16)
```

```python
import functools

import jax
import jax.numpy as jnp
from jax import lax
from jax.experimental import pallas as pl
from jax.experimental.pallas import tpu as pltpu
from jax.sharding import PartitionSpec as P

MESH = pl.DeviceIdType.MESH
VMEM = pltpu.VMEM
SMEM = pltpu.SMEM
DMA = pltpu.SemaphoreType.DMA
F32 = jnp.float32
BF16 = jnp.bfloat16


def across(c, d, n):
    out, bit = 0, 1
    while bit < n:
        out = out + bit * ((c // bit + d // bit) % 2)
        bit *= 2
    return out


def remote(src, dst, send, recv, to):
    return pltpu.make_async_remote_copy(
        src_ref=src, dst_ref=dst, send_sem=send, recv_sem=recv, device_id=to, device_id_type=MESH
    )


def greet(targets):
    barrier = pltpu.get_barrier_semaphore()
    for to in targets:
        pl.semaphore_signal(barrier, inc=1, device_id=to, device_id_type=MESH)
    pl.semaphore_wait(barrier, len(targets))


def shares(half_rows, chips):
    piece = max(half_rows * 3 // 4 // chips // 16, 1) * 16
    return piece, half_rows - piece * chips


def sigma_kernel(
    n_ops, n_blk, psi_hbm, left_hbm, r_hbm, target_ref, pair_ref, len_ref, out_ref,
    psi_v, left_in, stage, left_v, r_v, img, run, tab_v, tab_s, prev_s, last_s,
    part, recv1, sum1, recv_a1, recv_b1, send_a2, recv_a2, send_b2, recv_b2, send3, recv3,
    s_load, s_r, ss_a, sr_a, ss_c, sr_c, ss_l, sr_l, ss_z, sr_z, ss_y, ss_r, sr_r, ss_t, sr_t,
    ss_1, sr_1, ss_a1, sr_a1, ss_b1, sr_b1, ss_a2, sr_a2, ss_b2, sr_b2, ss_3, sr_3,
):
    g, c = lax.axis_index("ops"), lax.axis_index("blk")
    chips = n_ops // 2
    z, core = g // 2, g % 2
    partner = (z * 2 + (1 - core), c)
    peers = [across(c, d, n_blk) for d in range(n_blk)]
    order = list(range(1, n_blk))
    others = sorted(range(1, chips), key=lambda e: (abs(e * 2 - chips), e))

    half_rows, columns = psi_v.shape[1:]
    group, local_blocks, block_rows, _ = left_in.shape
    half_blocks = local_blocks // 2
    local_ops = r_hbm.shape[0]
    blocks = target_ref.shape[1]
    pairs = run.shape[0] - 1
    wide = r_v.shape[4]
    thin = wide // 2
    rest = n_blk // 2
    piece, straight = shares(half_rows, chips)

    def at_chip(e):
        return lax.rem(z + e, chips)

    mine = pl.ds(pl.multiple_of(core * half_rows, half_rows), half_rows)
    get_psi = pltpu.make_async_copy(psi_hbm.at[mine], psi_v.at[0], s_load.at[0])
    get_left = pltpu.make_async_copy(left_hbm, left_in, s_load.at[1])

    def get_r(j):
        return pltpu.make_async_copy(
            r_hbm.at[:, :, pl.ds(j * wide, wide)], r_v.at[0, j], s_r.at[j]
        )

    get_psi.start()
    get_left.start()
    for j in range(chips):
        get_r(j).start()

    greet(
        [partner]
        + [(z * 2 + k, peers[d]) for d in order for k in range(2)]
        + [(at_chip(e) * 2 + core, c) for e in range(1, chips)]
    )

    def rows_of(chip):
        return pl.ds(pl.multiple_of(chip * piece, piece), piece)

    rest_rows = pl.ds(piece * chips, straight)

    def first(d):
        return remote(
            psi_v.at[0, rows_of(z)], psi_v.at[d, rows_of(z)], ss_a.at[d], sr_a.at[d], (g, peers[d])
        )

    def plain(d):
        return remote(
            psi_v.at[0, rest_rows], psi_v.at[d, rest_rows], ss_c.at[d], sr_c.at[d], (g, peers[d])
        )

    def along(d, e):
        here = psi_v.at[d, rows_of(z)]
        return remote(here, here, ss_z.at[d, e], sr_z.at[d, z], (at_chip(e) * 2 + core, c))

    def passed(d, way):
        source, to = (0, chips - 1) if way == 0 else (chips - 1, 0)
        here = psi_v.at[d, rows_of(source)]
        return remote(here, here, ss_y.at[d, way], sr_z.at[d, source], (to * 2 + core, c))

    def arrived(d, source):
        here = psi_v.at[d, rows_of(source)]
        return remote(here, here, ss_z.at[d, 0], sr_z.at[d, source], partner)

    relay = chips > 2

    def near(e):
        if not relay:
            return True
        to = at_chip(e)
        return jnp.logical_and(to - z < chips - 1, z - to < chips - 1)

    def relays(way):
        return z == (chips - 2 if way == 0 else 1)

    def swap_r(j):
        return remote(r_v.at[0, j], r_v.at[1, j], ss_r.at[j], sr_r.at[j], partner)

    def lefts(d, k):
        which = core if k == 0 else 1 - core
        to = (z * 2 + which, peers[d])
        first_op = pl.multiple_of(peers[d] * local_ops, local_ops)
        return remote(
            stage.at[which, pl.ds(first_op, local_ops)], left_v.at[d, k],
            ss_l.at[d, k], sr_l.at[d, k], to,
        )

    table = remote(tab_v.at[0], tab_v.at[1], ss_t, sr_t, partner)

    get_psi.wait()
    for d in order:
        first(d).start()
    for d in order:
        if straight:
            plain(d).start()

    tab_v[0] = jnp.zeros_like(tab_v[0])
    for j in range(group):
        tab_v[0, j : j + 1, :blocks] = target_ref[pl.ds(lax.rem(pair_ref[j], group), 1), :]
    table.start()

    get_left.wait()
    lane = lax.broadcasted_iota(jnp.int32, (1, block_rows), 1)

    def put(j, carry):
        owner = lax.rem(pair_ref[j], group)
        for k in range(2):
            for i in range(half_blocks):
                b = k * half_blocks + i
                live = lane < len_ref[c * local_blocks + b]
                block = left_in[owner, b]
                stage[k, j, i] = jnp.where(live, block, jnp.zeros_like(block))
        return carry

    lax.fori_loop(0, group, put, 0)
    for d in order:
        for k in range(2):
            lefts(d, k).start()
    for j in range(chips):
        get_r(j).wait()
        swap_r(j).start()
    lefts(0, 1).start()
    left_v[0, 0] = stage[core, pl.ds(c * local_ops, local_ops)]
    run[pairs] = jnp.zeros_like(run[pairs])

    def image(d, k):
        def one(j, carry):
            for r in range(local_ops):
                out = jnp.dot(psi_v[d], r_v[k, j, r], preferred_element_type=F32)
                img[j, d, k, r] = out.astype(BF16).reshape(half_blocks, block_rows, wide)
            return carry

        lax.fori_loop(0, chips, one, 0)

    image(0, 0)
    for d in order:
        first(d).wait_recv()
        for e in others:
            @pl.when(near(e))
            def _(d=d, e=e):
                along(d, e).start()

    table.wait_recv()
    get_table = pltpu.make_async_copy(tab_v, tab_s, s_load.at[2])
    get_table.start()
    get_table.wait()

    def link(p, last):
        i = p % half_blocks
        r = p // half_blocks % local_ops
        k = p // (half_blocks * local_ops) % 2
        d = p // (half_blocks * local_ops * 2)
        q = across(c, d, n_blk) * local_blocks + core * half_blocks + i
        t = tab_s[k, c * local_ops + r, q]
        before = jnp.int32(pairs)
        for b in range(blocks):
            before = jnp.where(t == b, last[b], before)
        prev_s[p] = before
        return tuple(jnp.where(t == b, p, last[b]) for b in range(blocks))

    last = lax.fori_loop(0, pairs, link, (jnp.int32(pairs),) * blocks)
    for b in range(blocks):
        last_s[b] = last[b]

    def pass_on(d):
        for way in range(2 if relay else 0):
            @pl.when(relays(way))
            def _(way=way):
                arrived(d, 0 if way == 0 else chips - 1).wait_recv()
                passed(d, way).start()

    def settle(d):
        for e in range(1, chips):
            source = at_chip(e)
            done = False
            if relay:
                done = jnp.logical_or(
                    jnp.logical_and(relays(0), source == 0),
                    jnp.logical_and(relays(1), source == chips - 1),
                )

            @pl.when(jnp.logical_not(done))
            def _(source=source):
                arrived(d, source).wait_recv()
        if straight:
            plain(d).wait_recv()

    pass_on(1)
    for j in range(chips):
        swap_r(j).wait_recv()
    image(0, 1)
    for d in order:
        if d + 1 < n_blk:
            pass_on(d + 1)
        settle(d)
        for k in range(2):
            image(d, k)
    lefts(0, 1).wait_recv()
    for d in order:
        for k in range(2):
            lefts(d, k).wait_recv()

    def mix(n):
        j = at_chip(n + 1)

        def one(p, carry):
            i = p % half_blocks
            r = p // half_blocks % local_ops
            k = p // (half_blocks * local_ops) % 2
            d = p // (half_blocks * local_ops * 2)
            mixed = jnp.dot(left_v[d, k, r, i], img[j, d, k, r, i], preferred_element_type=F32)
            run[p] = run[prev_s[p]] + mixed
            return carry

        lax.fori_loop(0, pairs, one, 0, unroll=4)

        def emit(d, carry):
            for i in range(local_blocks):
                half, at = i // half_blocks, i % half_blocks
                slot = d % 2 * rest + d // 2 if half == 0 else d
                rows = pl.ds(at * block_rows, block_rows)
                kept = run[last_s[across(c, d, n_blk) * local_blocks + i]].astype(BF16)
                part[n, 0, half, slot, rows] = kept[:, :thin]
                part[n, 1, half, slot, rows] = kept[:, thin:]
            return carry

        lax.fori_loop(0, n_blk, emit, 0)
        swap(n).start()

    def swap(n):
        return remote(part.at[n, 1 - core], recv1.at[n], ss_1.at[n], sr_1.at[n], partner)

    def step_a1(n):
        return remote(
            sum1.at[n, 0, pl.ds(rest, rest)], recv_a1.at[n], ss_a1.at[n], sr_a1.at[n], (g, peers[1])
        )

    def step_b1(n, dy):
        return remote(
            sum1.at[n, 1, pl.ds(2 * dy, 2)], recv_b1.at[n, dy],
            ss_b1.at[n, dy], sr_b1.at[n, dy], (g, peers[2 * dy]),
        )

    def step_a2(n, dy):
        return remote(
            send_a2.at[n, dy], recv_a2.at[n, dy], ss_a2.at[n, dy], sr_a2.at[n, dy], (g, peers[2 * dy])
        )

    def step_b2(n):
        return remote(send_b2.at[n], recv_b2.at[n], ss_b2.at[n], sr_b2.at[n], (g, peers[1]))

    def last_step(n):
        return remote(
            send3.at[n], recv3.at[n], ss_3.at[n], sr_3.at[n], (at_chip(n + 1) * 2 + core, c)
        )

    def join(n):
        swap(n).wait_recv()

        def add(half, slots):
            both = part[n, core, half, slots].astype(F32) + recv1[n, half, slots].astype(F32)
            sum1[n, half, slots] = both.astype(BF16)

        add(0, pl.ds(rest, rest))
        step_a1(n).start()
        add(1, pl.ds(2, n_blk - 2))
        for dy in range(1, rest):
            step_b1(n, dy).start()
        add(0, pl.ds(0, rest))
        add(1, pl.ds(0, 2))

    def middle(n):
        step_a1(n).wait_recv()
        for dy in range(1, rest):
            both = sum1[n, 0, dy].astype(F32) + recv_a1[n, dy].astype(F32)
            send_a2[n, dy] = both.astype(BF16)
            step_a2(n, dy).start()
        both = sum1[n, 1, 1].astype(F32)
        for dy in range(1, rest):
            step_b1(n, dy).wait_recv()
            both += recv_b1[n, dy, 1].astype(F32)
        send_b2[n] = both.astype(BF16)
        step_b2(n).start()

    def finish(n):
        a = sum1[n, 0, 0].astype(F32) + recv_a1[n, 0].astype(F32)
        b = sum1[n, 1, 0].astype(F32)
        for dy in range(1, rest):
            step_a2(n, dy).wait_recv()
            a += recv_a2[n, dy].astype(F32)
            b += recv_b1[n, dy, 0].astype(F32)
        step_b2(n).wait_recv()
        b += recv_b2[n].astype(F32)
        if n < chips - 1:
            send3[n, 0] = a.astype(BF16)
            send3[n, 1] = b.astype(BF16)
            last_step(n).start()
            return
        for e in range(chips - 1):
            last_step(e).wait_recv()
            a += recv3[e, 0].astype(F32)
            b += recv3[e, 1].astype(F32)
        row = lax.broadcasted_iota(jnp.int32, (block_rows, 1), 0)
        for i in range(local_blocks):
            at = i % half_blocks * block_rows
            kept = (a if i < half_blocks else b)[at : at + block_rows]
            kept = jnp.where(row < len_ref[c * local_blocks + i], kept, jnp.zeros_like(kept))
            out_ref[i * block_rows : (i + 1) * block_rows] = kept.astype(out_ref.dtype)

    for n in range(chips + 3):
        if n < chips:
            mix(n)
        if 0 <= n - 1 < chips:
            join(n - 1)
        if 0 <= n - 2 < chips:
            middle(n - 2)
        if 0 <= n - 3 < chips:
            finish(n - 3)

    table.wait_send()
    lefts(0, 1).wait_send()
    for j in range(chips):
        swap_r(j).wait_send()
    for d in order:
        first(d).wait_send()
        if straight:
            plain(d).wait_send()
        for k in range(2):
            lefts(d, k).wait_send()
        for e in others:
            @pl.when(near(e))
            def _(d=d, e=e):
                along(d, e).wait_send()
        for way in range(2 if relay else 0):
            @pl.when(relays(way))
            def _(d=d, way=way):
                passed(d, way).wait_send()
    for n in range(chips):
        swap(n).wait_send()
        step_a1(n).wait_send()
        step_b2(n).wait_send()
        for dy in range(1, rest):
            step_b1(n, dy).wait_send()
            step_a2(n, dy).wait_send()
        if n < chips - 1:
            last_step(n).wait_send()


def local(n_ops, n_blk, psi, left_blocks, right_ops, block_target, left_partner, block_len):
    group, local_blocks, block_rows, _ = left_blocks.shape
    my_rows, columns = psi.shape
    local_ops = right_ops.shape[0]
    blocks = block_target.shape[1]
    chips = n_ops // 2
    thin = columns // n_ops
    wide = 2 * thin
    half_rows, half_blocks = my_rows // 2, local_blocks // 2
    rest = n_blk // 2
    pairs = n_blk * 2 * local_ops * half_blocks
    in_vmem = pl.BlockSpec(memory_space=pltpu.VMEM)
    in_smem = pl.BlockSpec(memory_space=pltpu.SMEM)
    in_hbm = pl.BlockSpec(memory_space=pl.ANY)

    def dmas(*shapes):
        return [DMA(shape) for shape in shapes for _ in range(2)]

    return pl.pallas_call(
        functools.partial(sigma_kernel, n_ops, n_blk),
        out_shape=jax.ShapeDtypeStruct((my_rows, thin), BF16),
        in_specs=[in_hbm, in_hbm, in_hbm, in_vmem, in_smem, in_smem],
        out_specs=in_vmem,
        scratch_shapes=[
            VMEM((n_blk, half_rows, columns), BF16),
            VMEM(left_blocks.shape, BF16),
            VMEM((2, group, half_blocks, block_rows, block_rows), BF16),
            VMEM((n_blk, 2, local_ops, half_blocks, block_rows, block_rows), BF16),
            VMEM((2, chips, local_ops, columns, wide), BF16),
            VMEM((chips, n_blk, 2, local_ops, half_blocks, block_rows, wide), BF16),
            VMEM((pairs + 1, block_rows, wide), F32),
            VMEM((2, group, 128), jnp.int32),
            SMEM((2, group, 128), jnp.int32),
            SMEM((pairs,), jnp.int32),
            SMEM((blocks,), jnp.int32),
            VMEM((chips, 2, 2, n_blk, half_rows, thin), BF16),
            VMEM((chips, 2, n_blk, half_rows, thin), BF16),
            VMEM((chips, 2, n_blk, half_rows, thin), BF16),
            VMEM((chips, rest, half_rows, thin), BF16),
            VMEM((chips, rest, 2, half_rows, thin), BF16),
            VMEM((chips, rest, half_rows, thin), BF16),
            VMEM((chips, rest, half_rows, thin), BF16),
            VMEM((chips, half_rows, thin), BF16),
            VMEM((chips, half_rows, thin), BF16),
            VMEM((chips, 2, half_rows, thin), BF16),
            VMEM((chips, 2, half_rows, thin), BF16),
            DMA((3,)), DMA((chips,)),
            *dmas((n_blk,), (n_blk,), (n_blk, 2), (n_blk, chips)),
            DMA((n_blk, 2)),
            *dmas((chips,), ()),
            *dmas((chips,), (chips,), (chips, rest), (chips, rest), (chips,), (chips,)),
        ],
        compiler_params=pltpu.CompilerParams(
            collective_id=0, has_side_effects=True, vmem_limit_bytes=63 * 2**20
        ),
        name="sigma",
    )(psi, left_blocks, right_ops, block_target, left_partner, block_len)


def solution(mesh):
    return jax.shard_map(
        functools.partial(local, mesh.shape["ops"], mesh.shape["blk"]),
        mesh=mesh,
        in_specs=(
            P("blk", None),
            P("ops", "blk", None, None),
            P(("ops", "blk"), None, None),
            P("ops", None),
            P("ops"),
            P(),
        ),
        out_specs=P("blk", "ops"),
        check_vma=False,
    )
```

```python
import functools

import jax
import jax.numpy as jnp
from jax import lax
from jax.experimental import pallas as pl
from jax.experimental.pallas import tpu as pltpu
from jax.sharding import PartitionSpec as P

MESH = pl.DeviceIdType.MESH
VMEM = pltpu.VMEM
SMEM = pltpu.SMEM
DMA = pltpu.SemaphoreType.DMA
F32 = jnp.float32
BF16 = jnp.bfloat16
scope = jax.named_scope


def across(c, d, n):
    out, bit = 0, 1
    while bit < n:
        out = out + bit * ((c // bit + d // bit) % 2)
        bit *= 2
    return out


def remote(src, dst, send, recv, to):
    return pltpu.make_async_remote_copy(
        src_ref=src, dst_ref=dst, send_sem=send, recv_sem=recv, device_id=to, device_id_type=MESH
    )


def shares(half_rows, chips):
    sizes = [max(half_rows // 2 // chips // 16, 1) * 16] * chips
    return sizes, [sum(sizes[:n]) for n in range(chips)]


def sigma_kernel(
    n_ops, n_blk, psi_hbm, left_hbm, r_hbm, target_ref, pair_ref, len_ref, out_ref,
    psi_v, left_in, stage, left_v, r_v, img, run, tab_v, tab_s, prev_s, last_s,
    part, recv1, sum1, recv_a1, recv_b1, send_a2, recv_a2, send_b2, recv_b2, send3, recv3,
    s_load, s_r, ss_a, sr_a, ss_c, sr_c, ss_f, sr_f, ss_g, sr_g, ss_l, sr_l, ss_z, sr_z, ss_y, above, ss_r, sr_r, ss_t, sr_t,
    ss_1, sr_1, ss_a1, sr_a1, ss_b1, sr_b1, ss_a2, sr_a2, ss_b2, sr_b2, ss_3, sr_3,
):
    g, c = lax.axis_index("ops"), lax.axis_index("blk")
    chips = n_ops // 2
    z, core = g // 2, g % 2
    partner = (z * 2 + (1 - core), c)
    peers = [across(c, d, n_blk) for d in range(n_blk)]
    order = list(range(1, n_blk))

    half_rows, columns = psi_v.shape[1:]
    group, local_blocks, block_rows, _ = left_in.shape
    half_blocks = local_blocks // 2
    local_ops = r_hbm.shape[0]
    thin = out_ref.shape[1]
    wide = 2 * thin
    blocks = target_ref.shape[1]
    pairs = run.shape[0] - 1
    rest = n_blk // 2
    sizes, starts = shares(half_rows, chips)
    plain_start = sum(sizes)
    straight = half_rows - plain_start

    def facing(n):
        return across(z, chips - 1 - n, chips)

    mine = pl.ds(pl.multiple_of(core * half_rows, half_rows), half_rows)
    get_psi = pltpu.make_async_copy(psi_hbm.at[mine], psi_v.at[0], s_load.at[0])
    get_left = pltpu.make_async_copy(left_hbm, left_in, s_load.at[1])

    def get_r(r):
        return pltpu.make_async_copy(r_hbm.at[r], r_v.at[0, r], s_r.at[r])

    get_psi.start()

    def by_chip(run_one):
        for chip in range(chips):
            @pl.when(z == chip)
            def _(chip=chip):
                run_one(chip)

    barrier = pltpu.get_barrier_semaphore()
    plane = [partner] + [(z * 2 + k, peers[d]) for d in order for k in range(2)]
    for to in plane:
        pl.semaphore_signal(barrier, inc=1, device_id=to, device_id_type=MESH)
    for e in range(1, chips):
        @pl.when(z + e < chips)
        def _(e=e):
            to = (g + 2 * e, c)
            pl.semaphore_signal(barrier, inc=1, device_id=to, device_id_type=MESH)
    with scope("greet"):
        by_chip(lambda chip: pl.semaphore_wait(barrier, len(plane) + chip))
    for e in range(1, chips):
        @pl.when(z >= e)
        def _(e=e):
            to = (g - 2 * e, c)
            pl.semaphore_signal(above.at[z], inc=1, device_id=to, device_id_type=MESH)

    def rows_of(chip):
        return pl.ds(starts[chip], sizes[chip])

    rest_rows = pl.ds(plain_start, straight)

    near_d = [1] + list(range(2, n_blk, 2))
    far_d = list(range(3, n_blk, 2))

    def first(d, chip):
        rows = rows_of(chip)
        return remote(
            psi_v.at[0, rows], psi_v.at[d, rows], ss_a.at[d], sr_a.at[d], (g, peers[d])
        )

    def plain(d):
        return remote(
            psi_v.at[0, rest_rows], psi_v.at[d, rest_rows], ss_c.at[d], sr_c.at[d], (g, peers[d])
        )

    def second(d, way, chip):
        source, to = (d - 1, 1) if way == 0 else (1, d - 1)
        at = pl.ds(starts[chip] + way * (sizes[chip] // 2), sizes[chip] // 2)
        return remote(
            psi_v.at[source, at], psi_v.at[d, at], ss_f.at[d, way], sr_f.at[d, way], (g, peers[to])
        )

    def plain_second(d, way):
        source, to = (d - 1, 1) if way == 0 else (1, d - 1)
        at = pl.ds(plain_start + way * (straight // 2), straight // 2)
        return remote(
            psi_v.at[source, at], psi_v.at[d, at], ss_g.at[d, way], sr_g.at[d, way], (g, peers[to])
        )

    def along(d, chip, to):
        here = psi_v.at[d, rows_of(chip)]
        return remote(here, here, ss_z.at[d, to], sr_z.at[d, chip], (to * 2 + core, c))

    def passed(d, source, to):
        here = psi_v.at[d, rows_of(source)]
        return remote(here, here, ss_y.at[d, source], sr_z.at[d, source], (to * 2 + core, c))

    def arrived(d, source):
        here = psi_v.at[d, rows_of(source)]
        return remote(here, here, ss_z.at[d, 0], sr_z.at[d, source], partner)

    relays = []
    if chips > 2:
        relays.append((chips - 2, list(range(chips - 3, -1, -1)), chips - 1))
        relays.append((1, list(range(2, chips)), 0))

    def targets(chip):
        skip = [to for _, sources, to in relays if chip in sources]
        found = [to for to in range(chips) if to != chip and to not in skip]
        return sorted(found, key=lambda to: -abs(to - chip))

    def swap_r(r):
        return remote(r_v.at[0, r], r_v.at[1, r], ss_r.at[r], sr_r.at[r], partner)

    def lefts(d, k):
        which = core if k == 0 else 1 - core
        to = (z * 2 + which, peers[d])
        first_op = pl.multiple_of(peers[d] * local_ops, local_ops)
        return remote(
            stage.at[which, pl.ds(first_op, local_ops)], left_v.at[d, k],
            ss_l.at[d, k], sr_l.at[d, k], to,
        )

    table = remote(tab_v.at[0], tab_v.at[1], ss_t, sr_t, partner)

    def start_plane(chip):
        for d in near_d:
            first(d, chip).start()

    with scope("psi"):
        get_psi.wait()
        get_left.start()
    with scope("start_plane"):
        by_chip(start_plane)
        for d in near_d:
            if straight:
                plain(d).start()
    for r in range(local_ops):
        get_r(r).start()

    tab_v[0] = jnp.zeros_like(tab_v[0])
    for j in range(group):
        tab_v[0, j : j + 1, :blocks] = target_ref[pl.ds(lax.rem(pair_ref[j], group), 1), :]
    table.start()

    with scope("left"):
        get_left.wait()
    lane = lax.broadcasted_iota(jnp.int32, (1, block_rows), 1)

    def put(j, carry):
        owner = lax.rem(pair_ref[j], group)
        for k in range(2):
            for i in range(half_blocks):
                b = k * half_blocks + i
                live = lane < len_ref[c * local_blocks + b]
                block = left_in[owner, b]
                stage[k, j, i] = jnp.where(live, block, jnp.zeros_like(block))
        return carry

    lax.fori_loop(0, group, put, 0)
    def spread_near(chip):
        first(1, chip).wait_recv()
        for f in far_d:
            second(f, 1, chip).start()
        for d in near_d[1:]:
            first(d, chip).wait_recv()
            second(d + 1, 0, chip).start()
        for to in range(chip + 1, chips):
            pl.semaphore_wait(above.at[to], 1)
        for d in near_d:
            for to in targets(chip):
                along(d, chip, to).start()

    with scope("spread_near"):
        by_chip(spread_near)
    for d in near_d:
        for k in range(2):
            lefts(d, k).start()
    for r in range(local_ops):
        get_r(r).wait()
        swap_r(r).start()
    lefts(0, 1).start()
    left_v[0, 0] = stage[core, pl.ds(c * local_ops, local_ops)]
    run[pairs] = jnp.zeros_like(run[pairs])

    def image(d, k):
        def one(r, carry):
            out = jnp.dot(psi_v[d], r_v[k, r], preferred_element_type=F32).astype(BF16)
            for j in range(chips):
                piece = out[:, j * wide : (j + 1) * wide]
                img[j, d, k, r] = piece.reshape(half_blocks, block_rows, wide)
            return carry

        lax.fori_loop(0, local_ops, one, 0)

    with scope("image00"):
        image(0, 0)
    table.wait_recv()
    get_table = pltpu.make_async_copy(tab_v, tab_s, s_load.at[2])
    get_table.start()
    get_table.wait()

    def link(p, last):
        i = p % half_blocks
        r = p // half_blocks % local_ops
        k = p // (half_blocks * local_ops) % 2
        d = p // (half_blocks * local_ops * 2)
        q = across(c, d, n_blk) * local_blocks + core * half_blocks + i
        t = tab_s[k, c * local_ops + r, q]
        before = jnp.int32(pairs)
        for b in range(blocks):
            before = jnp.where(t == b, last[b], before)
        prev_s[p] = before
        return tuple(jnp.where(t == b, p, last[b]) for b in range(blocks))

    with scope("link"):
        last = lax.fori_loop(0, pairs, link, (jnp.int32(pairs),) * blocks)
    for b in range(blocks):
        last_s[b] = last[b]

    with scope("plain_near"):
        for d in near_d:
            if straight:
                plain(d).wait_recv()
            for f in far_d:
                if straight and (d == 1 or d == f - 1):
                    plain_second(f, 1 if d == 1 else 0).start()
    for d in far_d:
        for k in range(2):
            lefts(d, k).start()

    def spread_far(chip):
        for d in far_d:
            for way in range(2):
                second(d, way, chip).wait_recv()
            for to in targets(chip):
                along(d, chip, to).start()

    with scope("spread_far"):
        by_chip(spread_far)

    def pass_on(d):
        for node, sources, to in relays:
            @pl.when(z == node)
            def _(sources=sources, to=to):
                for source in sources:
                    arrived(d, source).wait_recv()
                    passed(d, source, to).start()

    def settle(d):
        for source in range(chips):
            due = z != source
            for node, sources, _ in relays:
                if source in sources:
                    due = jnp.logical_and(due, z != node)

            @pl.when(due)
            def _(source=source):
                arrived(d, source).wait_recv()
        if straight and d in far_d:
            for way in range(2):
                plain_second(d, way).wait_recv()

    with scope("pass#d=1"):
        pass_on(1)
    with scope("swapr"):
        for r in range(local_ops):
            swap_r(r).wait_recv()
    with scope("image01"):
        image(0, 1)
    for d in order:
        if d + 1 < n_blk:
            with scope("pass#d=%d" % (d + 1)):
                pass_on(d + 1)
        with scope("settle#d=%d" % d):
            settle(d)
        with scope("image#d=%d" % d):
            image(d, 0)
            image(d, 1)

    def mix(n):
        j = facing(n)

        def one(p, carry):
            i = p % half_blocks
            r = p // half_blocks % local_ops
            k = p // (half_blocks * local_ops) % 2
            d = p // (half_blocks * local_ops * 2)
            mixed = jnp.dot(left_v[d, k, r, i], img[j, d, k, r, i], preferred_element_type=F32)
            run[p] = run[prev_s[p]] + mixed
            return carry

        if n == 0:
            each = pairs // n_blk
            lefts(0, 1).wait_recv()
            for d in range(n_blk):
                for k in range(2 if d else 0):
                    lefts(d, k).wait_recv()
                lax.fori_loop(d * each, (d + 1) * each, one, 0, unroll=min(each, 8))
        else:
            lax.fori_loop(0, pairs, one, 0, unroll=8)

        def emit(d, carry):
            for i in range(local_blocks):
                half, at = i // half_blocks, i % half_blocks
                slot = d % 2 * rest + d // 2 if half == 0 else d
                rows = pl.ds(at * block_rows, block_rows)
                kept = run[last_s[across(c, d, n_blk) * local_blocks + i]].astype(BF16)
                part[n, 0, half, slot, rows] = kept[:, :thin]
                part[n, 1, half, slot, rows] = kept[:, thin:]
            return carry

        lax.fori_loop(0, n_blk, emit, 0)
        swap(n).start()

    def swap(n):
        return remote(part.at[n, 1 - core], recv1.at[n], ss_1.at[n], sr_1.at[n], partner)

    def step_a1(n):
        return remote(
            sum1.at[n, 0, pl.ds(rest, rest)], recv_a1.at[n], ss_a1.at[n], sr_a1.at[n], (g, peers[1])
        )

    def step_b1(n, dy):
        return remote(
            sum1.at[n, 1, pl.ds(2 * dy, 2)], recv_b1.at[n, dy],
            ss_b1.at[n, dy], sr_b1.at[n, dy], (g, peers[2 * dy]),
        )

    def step_a2(n, dy):
        return remote(
            send_a2.at[n, dy], recv_a2.at[n, dy], ss_a2.at[n, dy], sr_a2.at[n, dy], (g, peers[2 * dy])
        )

    def step_b2(n):
        return remote(send_b2.at[n], recv_b2.at[n], ss_b2.at[n], sr_b2.at[n], (g, peers[1]))

    def last_step(n):
        return remote(
            send3.at[n], recv3.at[n], ss_3.at[n], sr_3.at[n], (facing(n) * 2 + core, c)
        )

    def join(n):
        swap(n).wait_recv()

        def add(half, slots):
            both = part[n, core, half, slots].astype(F32) + recv1[n, half, slots].astype(F32)
            sum1[n, half, slots] = both.astype(BF16)

        add(0, pl.ds(rest, rest))
        step_a1(n).start()
        add(1, pl.ds(2, n_blk - 2))
        for dy in range(1, rest):
            step_b1(n, dy).start()
        add(0, pl.ds(0, rest))
        add(1, pl.ds(0, 2))

    def middle(n):
        step_a1(n).wait_recv()
        for dy in range(1, rest):
            both = sum1[n, 0, dy].astype(F32) + recv_a1[n, dy].astype(F32)
            send_a2[n, dy] = both.astype(BF16)
            step_a2(n, dy).start()
        both = sum1[n, 1, 1].astype(F32)
        for dy in range(1, rest):
            step_b1(n, dy).wait_recv()
            both += recv_b1[n, dy, 1].astype(F32)
        send_b2[n] = both.astype(BF16)
        step_b2(n).start()

    def finish(n):
        a = sum1[n, 0, 0].astype(F32) + recv_a1[n, 0].astype(F32)
        b = sum1[n, 1, 0].astype(F32)
        for dy in range(1, rest):
            step_a2(n, dy).wait_recv()
            a += recv_a2[n, dy].astype(F32)
            b += recv_b1[n, dy, 0].astype(F32)
        step_b2(n).wait_recv()
        b += recv_b2[n].astype(F32)
        if n < chips - 1:
            send3[n, 0] = a.astype(BF16)
            send3[n, 1] = b.astype(BF16)
            last_step(n).start()
            return
        for e in range(chips - 1):
            last_step(e).wait_recv()
            a += recv3[e, 0].astype(F32)
            b += recv3[e, 1].astype(F32)
        row = lax.broadcasted_iota(jnp.int32, (block_rows, 1), 0)
        for i in range(local_blocks):
            at = i % half_blocks * block_rows
            kept = (a if i < half_blocks else b)[at : at + block_rows]
            kept = jnp.where(row < len_ref[c * local_blocks + i], kept, jnp.zeros_like(kept))
            out_ref[i * block_rows : (i + 1) * block_rows] = kept.astype(out_ref.dtype)

    def perform(stage_of, n):
        with scope("%s#n=%d" % (stage_of.__name__, n)):
            stage_of(n)

    perform(mix, 0)
    for n in range(1, chips):
        perform(mix, n)
        if n < 3:
            perform(join, n - 1)
    for n in range(chips):
        perform(middle, n)
        if n:
            perform(finish, n - 1)
        if 2 <= n + 2 < chips:
            perform(join, n + 2)
    perform(finish, chips - 1)

    table.wait_send()
    lefts(0, 1).wait_send()
    for r in range(local_ops):
        swap_r(r).wait_send()

    def drain(chip):
        for d in near_d:
            first(d, chip).wait_send()
        for d in far_d:
            for way in range(2):
                second(d, way, chip).wait_send()
        for d in order:
            for to in targets(chip):
                along(d, chip, to).wait_send()

    by_chip(drain)
    for d in order:
        for node, sources, to in relays:
            @pl.when(z == node)
            def _(d=d, sources=sources, to=to):
                for source in sources:
                    passed(d, source, to).wait_send()
        for k in range(2):
            lefts(d, k).wait_send()
    for d in near_d if straight else []:
        plain(d).wait_send()
    for d in far_d if straight else []:
        for way in range(2):
            plain_second(d, way).wait_send()
    for n in range(chips):
        swap(n).wait_send()
        step_a1(n).wait_send()
        step_b2(n).wait_send()
        for dy in range(1, rest):
            step_b1(n, dy).wait_send()
            step_a2(n, dy).wait_send()
        if n < chips - 1:
            last_step(n).wait_send()


def local(n_ops, n_blk, psi, left_blocks, right_ops, block_target, left_partner, block_len):
    group, local_blocks, block_rows, _ = left_blocks.shape
    my_rows, columns = psi.shape
    local_ops = right_ops.shape[0]
    blocks = block_target.shape[1]
    chips = n_ops // 2
    thin = columns // n_ops
    wide = 2 * thin
    half_rows, half_blocks = my_rows // 2, local_blocks // 2
    rest = n_blk // 2
    pairs = n_blk * 2 * local_ops * half_blocks
    in_vmem = pl.BlockSpec(memory_space=pltpu.VMEM)
    in_smem = pl.BlockSpec(memory_space=pltpu.SMEM)
    in_hbm = pl.BlockSpec(memory_space=pl.ANY)

    def dmas(*shapes):
        return [DMA(shape) for shape in shapes for _ in range(2)]

    return pl.pallas_call(
        functools.partial(sigma_kernel, n_ops, n_blk),
        out_shape=pltpu.VMEM((my_rows, thin), BF16),
        in_specs=[in_hbm, in_hbm, in_hbm, in_vmem, in_smem, in_smem],
        out_specs=in_vmem,
        scratch_shapes=[
            VMEM((n_blk, half_rows, columns), BF16),
            VMEM(left_blocks.shape, BF16),
            VMEM((2, group, half_blocks, block_rows, block_rows), BF16),
            VMEM((n_blk, 2, local_ops, half_blocks, block_rows, block_rows), BF16),
            VMEM((2, local_ops, columns, columns), BF16),
            VMEM((chips, n_blk, 2, local_ops, half_blocks, block_rows, wide), BF16),
            VMEM((pairs + 1, block_rows, wide), F32),
            VMEM((2, group, 128), jnp.int32),
            SMEM((2, group, 128), jnp.int32),
            SMEM((pairs,), jnp.int32),
            SMEM((blocks,), jnp.int32),
            VMEM((chips, 2, 2, n_blk, half_rows, thin), BF16),
            VMEM((chips, 2, n_blk, half_rows, thin), BF16),
            VMEM((chips, 2, n_blk, half_rows, thin), BF16),
            VMEM((chips, rest, half_rows, thin), BF16),
            VMEM((chips, rest, 2, half_rows, thin), BF16),
            VMEM((chips, rest, half_rows, thin), BF16),
            VMEM((chips, rest, half_rows, thin), BF16),
            VMEM((chips, half_rows, thin), BF16),
            VMEM((chips, half_rows, thin), BF16),
            VMEM((chips, 2, half_rows, thin), BF16),
            VMEM((chips, 2, half_rows, thin), BF16),
            DMA((3,)), DMA((local_ops,)),
            *dmas((n_blk,), (n_blk,), (n_blk, 2), (n_blk, 2), (n_blk, 2), (n_blk, chips)),
            DMA((n_blk, chips)), pltpu.SemaphoreType.REGULAR((chips,)),
            *dmas((local_ops,), ()),
            *dmas((chips,), (chips,), (chips, rest), (chips, rest), (chips,), (chips,)),
        ],
        compiler_params=pltpu.CompilerParams(
            collective_id=0, has_side_effects=True, vmem_limit_bytes=63 * 2**20
        ),
        name="sigma",
    )(psi, left_blocks, right_ops, block_target, left_partner, block_len)


def solution(mesh):
    return jax.shard_map(
        functools.partial(local, mesh.shape["ops"], mesh.shape["blk"]),
        mesh=mesh,
        in_specs=(
            P("blk", None),
            P("ops", "blk", None, None),
            P(("ops", "blk"), None, None),
            P("ops", None),
            P("ops"),
            P(),
        ),
        out_specs=P("blk", "ops"),
        check_vma=False,
    )
```

```python
import functools

import jax
import jax.numpy as jnp
from jax import lax
from jax.experimental import pallas as pl
from jax.experimental.pallas import tpu as pltpu
from jax.sharding import PartitionSpec as P

MESH = pl.DeviceIdType.MESH
VMEM = pltpu.VMEM
SMEM = pltpu.SMEM
DMA = pltpu.SemaphoreType.DMA
F32 = jnp.float32
BF16 = jnp.bfloat16
scope = jax.named_scope


def across(c, d, n):
    out, bit = 0, 1
    while bit < n:
        out = out + bit * ((c // bit + d // bit) % 2)
        bit *= 2
    return out


def remote(src, dst, send, recv, to):
    return pltpu.make_async_remote_copy(
        src_ref=src, dst_ref=dst, send_sem=send, recv_sem=recv, device_id=to, device_id_type=MESH
    )


def shares(half_rows, chips):
    sizes = [max(half_rows // 2 // chips // 16, 1) * 16] * chips
    return sizes, [sum(sizes[:n]) for n in range(chips)]


def sigma_kernel(
    n_ops, n_blk, psi_hbm, left_hbm, r_hbm, target_ref, pair_ref, len_ref, out_ref,
    own, psi_z, psi_p, left_in, stage, left_v, r_v, img, run, tab_v, tab_s, prev_s, last_s,
    part, recv1, sum1, recv_z, recv_a1, recv_b1, send_a2, recv_a2, send_b2, recv_b2, send3, recv3,
    s_load, s_r, ss_a, sr_a, ss_c, sr_c, ss_f, sr_f, ss_g, sr_g, ss_l, sr_l, ss_z, sr_z, ss_y, above, ss_r, sr_r, ss_t, sr_t,
    ss_1, sr_1, ss_f1, sr_f1, ss_a1, sr_a1, ss_b1, sr_b1, ss_a2, sr_a2, ss_b2, sr_b2, ss_3, sr_3,
):
    g, c = lax.axis_index("ops"), lax.axis_index("blk")
    chips = n_ops // 2
    z, core = g // 2, g % 2
    partner = (z * 2 + (1 - core), c)
    peers = [across(c, d, n_blk) for d in range(n_blk)]
    order = list(range(1, n_blk))

    columns = psi_hbm.shape[1]
    half_rows = psi_hbm.shape[0] // 2
    group, local_blocks, block_rows, _ = left_in.shape
    half_blocks = local_blocks // 2
    local_ops = r_hbm.shape[0]
    thin = out_ref.shape[1]
    wide = 2 * thin
    blocks = target_ref.shape[1]
    pairs = run.shape[0] - 1
    rest = n_blk // 2
    sizes, starts = shares(half_rows, chips)
    climb = sum(sizes)
    straight = half_rows - climb
    ahead = recv_z.shape[3]

    def facing(n):
        return across(z, chips - 1 - n, chips)

    mine = pl.ds(pl.multiple_of(core * half_rows, half_rows), half_rows)
    get_psi = pltpu.make_async_copy(psi_hbm.at[mine], own, s_load.at[0])
    get_left = pltpu.make_async_copy(left_hbm, left_in, s_load.at[1])

    def get_r(r):
        return pltpu.make_async_copy(r_hbm.at[r], r_v.at[0, r], s_r.at[r])

    get_psi.start()

    def by_chip(run_one):
        for chip in range(chips):
            @pl.when(z == chip)
            def _(chip=chip):
                run_one(chip)

    barrier = pltpu.get_barrier_semaphore()
    plane = [partner] + [(z * 2 + k, peers[d]) for d in order for k in range(2)]
    for to in plane:
        pl.semaphore_signal(barrier, inc=1, device_id=to, device_id_type=MESH)
    for e in range(1, chips):
        @pl.when(z + e < chips)
        def _(e=e):
            to = (g + 2 * e, c)
            pl.semaphore_signal(barrier, inc=1, device_id=to, device_id_type=MESH)
    with scope("greet"):
        by_chip(lambda chip: pl.semaphore_wait(barrier, len(plane) + chip))
    for e in range(1, chips):
        @pl.when(z >= e)
        def _(e=e):
            to = (g - 2 * e, c)
            pl.semaphore_signal(above.at[z], inc=1, device_id=to, device_id_type=MESH)

    def rows_of(chip):
        return pl.ds(starts[chip], sizes[chip])

    near_d = [1] + list(range(2, n_blk, 2))
    far_d = list(range(3, n_blk, 2))

    def first(d, chip):
        rows = rows_of(chip)
        return remote(
            own.at[rows], psi_z.at[d, rows], ss_a.at[d], sr_a.at[d], (g, peers[d])
        )

    def plain(d):
        return remote(
            own.at[pl.ds(climb, straight)], psi_p.at[d], ss_c.at[d], sr_c.at[d], (g, peers[d])
        )

    def second(d, way, chip):
        source, to = (d - 1, 1) if way == 0 else (1, d - 1)
        at = pl.ds(starts[chip] + way * (sizes[chip] // 2), sizes[chip] // 2)
        return remote(
            psi_z.at[source, at], psi_z.at[d, at], ss_f.at[d, way], sr_f.at[d, way], (g, peers[to])
        )

    def plain_second(d, way):
        source, to = (d - 1, 1) if way == 0 else (1, d - 1)
        at = pl.ds(way * (straight // 2), straight // 2)
        return remote(
            psi_p.at[source, at], psi_p.at[d, at], ss_g.at[d, way], sr_g.at[d, way], (g, peers[to])
        )

    def along(d, chip, to):
        here = psi_z.at[d, rows_of(chip)]
        return remote(here, here, ss_z.at[d, to], sr_z.at[d, chip], (to * 2 + core, c))

    def passed(d, source, to):
        here = psi_z.at[d, rows_of(source)]
        return remote(here, here, ss_y.at[d, source], sr_z.at[d, source], (to * 2 + core, c))

    def arrived(d, source):
        here = psi_z.at[d, rows_of(source)]
        return remote(here, here, ss_z.at[d, 0], sr_z.at[d, source], partner)

    relays = []
    if chips > 2:
        relays.append((chips - 2, [0], chips - 1))
        relays.append((1, [chips - 1], 0))

    def targets(chip):
        skip = [to for _, sources, to in relays if chip in sources]
        found = [to for to in range(chips) if to != chip and to not in skip]
        return sorted(found, key=lambda to: -abs(to - chip))

    def swap_r(r):
        return remote(r_v.at[0, r], r_v.at[1, r], ss_r.at[r], sr_r.at[r], partner)

    def lefts(d, k):
        which = core if k == 0 else 1 - core
        to = (z * 2 + which, peers[d])
        first_op = pl.multiple_of(peers[d] * local_ops, local_ops)
        return remote(
            stage.at[which, pl.ds(first_op, local_ops)], left_v.at[d, k],
            ss_l.at[d, k], sr_l.at[d, k], to,
        )

    table = remote(tab_v.at[0], tab_v.at[1], ss_t, sr_t, partner)

    def start_plane(chip):
        for d in near_d:
            first(d, chip).start()

    with scope("psi"):
        get_psi.wait()
        get_left.start()
    with scope("start_plane"):
        by_chip(start_plane)
        for d in near_d:
            if straight:
                plain(d).start()
    for r in range(local_ops):
        get_r(r).start()

    tab_v[0] = jnp.zeros_like(tab_v[0])
    for j in range(group):
        tab_v[0, j : j + 1, :blocks] = target_ref[pl.ds(lax.rem(pair_ref[j], group), 1), :]
    table.start()

    with scope("left"):
        get_left.wait()
    lane = lax.broadcasted_iota(jnp.int32, (1, block_rows), 1)

    def put(j, carry):
        owner = lax.rem(pair_ref[j], group)
        for k in range(2):
            for i in range(half_blocks):
                b = k * half_blocks + i
                live = lane < len_ref[c * local_blocks + b]
                block = left_in[owner, b]
                stage[k, j, i] = jnp.where(live, block, jnp.zeros_like(block))
        return carry

    lax.fori_loop(0, group, put, 0)
    def spread_near(chip):
        first(1, chip).wait_recv()
        for f in far_d:
            second(f, 1, chip).start()
        for d in near_d[1:]:
            first(d, chip).wait_recv()
            second(d + 1, 0, chip).start()
        for to in range(chip + 1, chips):
            pl.semaphore_wait(above.at[to], 1)
        for d in near_d:
            for to in targets(chip):
                along(d, chip, to).start()

    with scope("spread_near"):
        by_chip(spread_near)
    for d in near_d:
        lefts(d, 0).start()
    for r in range(local_ops):
        get_r(r).wait()
        swap_r(r).start()
    lefts(0, 1).start()
    left_v[0, 0] = stage[core, pl.ds(c * local_ops, local_ops)]
    run[pairs] = jnp.zeros_like(run[pairs])

    def image(state, first_d, count, at, k):
        rows = state.shape[0] // count

        def one(r, carry):
            out = jnp.dot(state[...], r_v[k, r], preferred_element_type=F32).astype(BF16)
            for d in range(count):
                for j in range(chips):
                    img[j, first_d + d, k, r, at : at + rows] = out[
                        d * rows : (d + 1) * rows, j * wide : (j + 1) * wide
                    ]
            return carry

        lax.fori_loop(0, local_ops, one, 0)

    def image_z(first_d, count, k):
        image(psi_z[first_d : first_d + count].reshape(count * climb, columns), first_d, count, 0, k)

    def image_p(first_d, count, k):
        if straight:
            state = psi_p[first_d : first_d + count].reshape(count * straight, columns)
            image(state, first_d, count, climb, k)

    with scope("image00"):
        image(own, 0, 1, 0, 0)
    table.wait_recv()
    get_table = pltpu.make_async_copy(tab_v, tab_s, s_load.at[2])
    get_table.start()
    get_table.wait()

    def link(p, last):
        i = p % half_blocks
        r = p // half_blocks % local_ops
        k = p // (half_blocks * local_ops) % 2
        d = p // (half_blocks * local_ops * 2)
        q = across(c, d, n_blk) * local_blocks + core * half_blocks + i
        t = tab_s[k, c * local_ops + r, q]
        before = jnp.int32(pairs)
        for b in range(blocks):
            before = jnp.where(t == b, last[b], before)
        prev_s[p] = before
        return tuple(jnp.where(t == b, p, last[b]) for b in range(blocks))

    with scope("link"):
        last = lax.fori_loop(0, pairs, link, (jnp.int32(pairs),) * blocks)
    for b in range(blocks):
        last_s[b] = last[b]

    with scope("plain_near"):
        for d in near_d:
            if straight:
                plain(d).wait_recv()
            for f in far_d:
                if straight and (d == 1 or d == f - 1):
                    plain_second(f, 1 if d == 1 else 0).start()
    for d in near_d:
        lefts(d, 1).start()
    for d in far_d:
        for k in range(2):
            lefts(d, k).start()

    def spread_far(chip):
        for d in far_d:
            for way in range(2):
                second(d, way, chip).wait_recv()
            for to in targets(chip):
                along(d, chip, to).start()

    with scope("spread_far"):
        by_chip(spread_far)

    def pass_on(d):
        for node, sources, to in relays:
            @pl.when(z == node)
            def _(sources=sources, to=to):
                for source in sources:
                    arrived(d, source).wait_recv()
                    passed(d, source, to).start()

    def settle(d):
        for source in range(chips):
            due = z != source
            for node, sources, _ in relays:
                if source in sources:
                    due = jnp.logical_and(due, z != node)

            @pl.when(due)
            def _(source=source):
                arrived(d, source).wait_recv()
    with scope("pass#d=1"):
        pass_on(1)
    with scope("swapr"):
        for r in range(local_ops):
            swap_r(r).wait_recv()
    with scope("image01"):
        image(own, 0, 1, 0, 1)
    tail_d = far_d[-1]
    for d in order[1:]:
        with scope("pass#d=%d" % d):
            pass_on(d)
        if d < tail_d and d % 2 == 0:
            with scope("image_p#d=%d" % d):
                for k in range(2):
                    image_p(d - 1, 2, k)
    with scope("plain_far"):
        for d in far_d if straight else []:
            for way in range(2):
                plain_second(d, way).wait_recv()
    with scope("image_p_far"):
        for k in range(2):
            image_p(tail_d, 1, k)
    for d in range(1, n_blk, 2):
        count = min(2, n_blk - d)
        with scope("settle#d=%d" % d):
            for e in range(count):
                settle(d + e)
        with scope("image_z#d=%d" % d):
            for k in range(2):
                image_z(d, count, k)

    def mix(n):
        j = facing(n)

        def one(p, carry):
            i = p % half_blocks
            r = p // half_blocks % local_ops
            k = p // (half_blocks * local_ops) % 2
            d = p // (half_blocks * local_ops * 2)
            rows = pl.ds(pl.multiple_of(i * block_rows, block_rows), block_rows)
            mixed = jnp.dot(left_v[d, k, r, i], img[j, d, k, r, rows], preferred_element_type=F32)
            run[p] = run[prev_s[p]] + mixed
            return carry

        if n == 0:
            each = pairs // n_blk
            lefts(0, 1).wait_recv()
            for d in range(n_blk):
                for k in range(2 if d else 0):
                    lefts(d, k).wait_recv()
                lax.fori_loop(d * each, (d + 1) * each, one, 0, unroll=min(each, 8))
        else:
            lax.fori_loop(0, pairs, one, 0, unroll=8)

        def emit(d, carry):
            for i in range(local_blocks):
                half, at = i // half_blocks, i % half_blocks
                slot = d % 2 * rest + d // 2 if half == 0 else d
                rows = pl.ds(at * block_rows, block_rows)
                kept = run[last_s[across(c, d, n_blk) * local_blocks + i]].astype(BF16)
                part[n, 0, half, slot, rows] = kept[:, :thin]
                part[n, 1, half, slot, rows] = kept[:, thin:]
            return carry

        lax.fori_loop(0, n_blk, emit, 0)
        swap(n).start()

    def swap(n):
        return remote(part.at[n, 1 - core], recv1.at[n], ss_1.at[n], sr_1.at[n], partner)

    early = pl.ds(0, ahead)
    late = pl.ds(ahead, half_rows - ahead)

    def moved(n):
        return early if n == chips else late

    def chunk(n):
        return min(n, chips - 1)

    def gathers(n):
        offset = chips - 1 - n
        return offset > 1 and offset % 2 == 1

    def step_z(n):
        return remote(
            sum1.at[n, :, :, early], recv_z.at[n], ss_f1.at[n], sr_f1.at[n], (facing(n) * 2 + core, c)
        )

    def step_a1(n):
        return remote(
            sum1.at[chunk(n), 0, pl.ds(rest, rest), moved(n)], recv_a1.at[chunk(n), :, moved(n)],
            ss_a1.at[n], sr_a1.at[n], (g, peers[1]),
        )

    def step_b1(n, dy):
        return remote(
            sum1.at[chunk(n), 1, pl.ds(2 * dy, 2), moved(n)], recv_b1.at[chunk(n), dy, :, moved(n)],
            ss_b1.at[n, dy], sr_b1.at[n, dy], (g, peers[2 * dy]),
        )

    def step_a2(n, dy):
        return remote(
            send_a2.at[chunk(n), dy, moved(n)], recv_a2.at[chunk(n), dy, moved(n)],
            ss_a2.at[n, dy], sr_a2.at[n, dy], (g, peers[2 * dy]),
        )

    def step_b2(n):
        return remote(
            send_b2.at[chunk(n), moved(n)], recv_b2.at[chunk(n), moved(n)],
            ss_b2.at[n], sr_b2.at[n], (g, peers[1]),
        )

    def last_step(n):
        return remote(
            send3.at[n, :, moved(n)], recv3.at[n, :, moved(n)],
            ss_3.at[n], sr_3.at[n], (facing(chips - 2 if gathers(n) else n) * 2 + core, c),
        )

    def add(n, half, slots):
        m, rows = chunk(n), moved(n)
        both = part[m, core, half, slots, rows].astype(F32) + recv1[m, half, slots, rows].astype(F32)
        if n == chips:
            for e in range(chips - 1):
                both += recv_z[e, half, slots].astype(F32)
        sum1[m, half, slots, rows] = both.astype(BF16)

    def begin(n):
        if n == 0:
            join(n)
        else:
            swap(n).wait_recv()
        for half in range(2):
            both = part[n, core, half, :, early].astype(F32) + recv1[n, half, :, early].astype(F32)
            sum1[n, half, :, early] = both.astype(BF16)
        step_z(n).start()

    def join(n):
        if n in (0, chips - 1):
            swap(n).wait_recv()
        if n == chips:
            for e in range(chips - 1):
                step_z(e).wait_recv()
        add(n, 0, pl.ds(rest, rest))
        step_a1(n).start()
        add(n, 1, pl.ds(2, n_blk - 2))
        for dy in range(1, rest):
            step_b1(n, dy).start()
        add(n, 0, pl.ds(0, rest))
        add(n, 1, pl.ds(0, 2))

    def middle(n):
        m, rows = chunk(n), moved(n)
        step_a1(n).wait_recv()
        for dy in range(1, rest):
            both = sum1[m, 0, dy, rows].astype(F32) + recv_a1[m, dy, rows].astype(F32)
            send_a2[m, dy, rows] = both.astype(BF16)
            step_a2(n, dy).start()
        both = sum1[m, 1, 1, rows].astype(F32)
        for dy in range(1, rest):
            step_b1(n, dy).wait_recv()
            both += recv_b1[m, dy, 1, rows].astype(F32)
        send_b2[m, rows] = both.astype(BF16)
        step_b2(n).start()

    row = lax.broadcasted_iota(jnp.int32, (block_rows, 1), 0)

    def put_out(half, value, first_row):
        size = value.shape[0]
        for i in range(half_blocks):
            low = max(first_row, i * block_rows)
            high = min(first_row + size, (i + 1) * block_rows)
            if low < high:
                kept = value[low - first_row : high - first_row]
                live = row[low - i * block_rows : high - i * block_rows] < len_ref[
                    c * local_blocks + half * half_blocks + i
                ]
                kept = jnp.where(live, kept, jnp.zeros_like(kept)).astype(out_ref.dtype)
                out_ref[half * half_rows + low : half * half_rows + high] = kept

    def finish(n):
        m, rows = chunk(n), moved(n)
        a = sum1[m, 0, 0, rows].astype(F32) + recv_a1[m, 0, rows].astype(F32)
        b = sum1[m, 1, 0, rows].astype(F32)
        for dy in range(1, rest):
            step_a2(n, dy).wait_recv()
            a += recv_a2[m, dy, rows].astype(F32)
            b += recv_b1[m, dy, 0, rows].astype(F32)
        step_b2(n).wait_recv()
        b += recv_b2[m, rows].astype(F32)
        if 0 < n < chips - 1 and gathers(n - 1):
            last_step(n - 1).wait_recv()
            a += recv3[n - 1, 0, rows].astype(F32)
            b += recv3[n - 1, 1, rows].astype(F32)
        if n < chips - 1:
            send3[n, 0, rows] = a.astype(BF16)
            send3[n, 1, rows] = b.astype(BF16)
            last_step(n).start()
            return
        if n == chips - 1:
            for e in [e for e in range(chips - 1) if not gathers(e)]:
                last_step(e).wait_recv()
                a += recv3[e, 0, rows].astype(F32)
                b += recv3[e, 1, rows].astype(F32)
        put_out(0, a, 0 if n == chips else ahead)
        put_out(1, b, 0 if n == chips else ahead)

    def perform(stage_of, n):
        with scope("%s#n=%d" % (stage_of.__name__, n)):
            stage_of(n)

    perform(mix, 0)
    for n in range(1, chips):
        perform(mix, n)
        perform(begin, n - 1)
        if n == 2:
            perform(join, 1)
    for n in range(chips):
        perform(middle, n)
        if n:
            perform(finish, n - 1)
        if 2 <= n + 2 < chips:
            perform(join, n + 2)
        if n == chips - 2:
            perform(join, chips)
    perform(middle, chips)
    perform(finish, chips)
    perform(finish, chips - 1)

    table.wait_send()
    lefts(0, 1).wait_send()
    for r in range(local_ops):
        swap_r(r).wait_send()

    def drain(chip):
        for d in near_d:
            first(d, chip).wait_send()
        for d in far_d:
            for way in range(2):
                second(d, way, chip).wait_send()
        for d in order:
            for to in targets(chip):
                along(d, chip, to).wait_send()

    by_chip(drain)
    for d in order:
        for node, sources, to in relays:
            @pl.when(z == node)
            def _(d=d, sources=sources, to=to):
                for source in sources:
                    passed(d, source, to).wait_send()
        for k in range(2):
            lefts(d, k).wait_send()
    for d in near_d if straight else []:
        plain(d).wait_send()
    for d in far_d if straight else []:
        for way in range(2):
            plain_second(d, way).wait_send()
    for n in range(chips - 1):
        step_z(n).wait_send()
    for n in range(chips):
        swap(n).wait_send()
        if n < chips - 1:
            last_step(n).wait_send()
    for n in range(chips + 1):
        step_a1(n).wait_send()
        step_b2(n).wait_send()
        for dy in range(1, rest):
            step_b1(n, dy).wait_send()
            step_a2(n, dy).wait_send()


def local(n_ops, n_blk, psi, left_blocks, right_ops, block_target, left_partner, block_len):
    group, local_blocks, block_rows, _ = left_blocks.shape
    my_rows, columns = psi.shape
    local_ops = right_ops.shape[0]
    blocks = block_target.shape[1]
    chips = n_ops // 2
    thin = columns // n_ops
    wide = 2 * thin
    half_rows, half_blocks = my_rows // 2, local_blocks // 2
    rest = n_blk // 2
    pairs = n_blk * 2 * local_ops * half_blocks
    in_vmem = pl.BlockSpec(memory_space=pltpu.VMEM)
    in_smem = pl.BlockSpec(memory_space=pltpu.SMEM)
    in_hbm = pl.BlockSpec(memory_space=pl.ANY)

    def dmas(*shapes):
        return [DMA(shape) for shape in shapes for _ in range(2)]

    return pl.pallas_call(
        functools.partial(sigma_kernel, n_ops, n_blk),
        out_shape=pltpu.VMEM((my_rows, thin), BF16),
        in_specs=[in_hbm, in_hbm, in_hbm, in_vmem, in_smem, in_smem],
        out_specs=in_vmem,
        scratch_shapes=[
            VMEM((half_rows, columns), BF16),
            VMEM((n_blk, sum(shares(half_rows, chips)[0]), columns), BF16),
            VMEM((n_blk, max(half_rows - sum(shares(half_rows, chips)[0]), 16), columns), BF16),
            VMEM(left_blocks.shape, BF16),
            VMEM((2, group, half_blocks, block_rows, block_rows), BF16),
            VMEM((n_blk, 2, local_ops, half_blocks, block_rows, block_rows), BF16),
            VMEM((2, local_ops, columns, columns), BF16),
            VMEM((chips, n_blk, 2, local_ops, half_rows, wide), BF16),
            VMEM((pairs + 1, block_rows, wide), F32),
            VMEM((2, group, 128), jnp.int32),
            SMEM((2, group, 128), jnp.int32),
            SMEM((pairs,), jnp.int32),
            SMEM((blocks,), jnp.int32),
            VMEM((chips, 2, 2, n_blk, half_rows, thin), BF16),
            VMEM((chips, 2, n_blk, half_rows, thin), BF16),
            VMEM((chips, 2, n_blk, half_rows, thin), BF16),
            VMEM((max(chips - 1, 1), 2, n_blk, max(half_rows * 3 // 16 // 16, 1) * 16, thin), BF16),
            VMEM((chips, rest, half_rows, thin), BF16),
            VMEM((chips, rest, 2, half_rows, thin), BF16),
            VMEM((chips, rest, half_rows, thin), BF16),
            VMEM((chips, rest, half_rows, thin), BF16),
            VMEM((chips, half_rows, thin), BF16),
            VMEM((chips, half_rows, thin), BF16),
            VMEM((chips, 2, half_rows, thin), BF16),
            VMEM((chips, 2, half_rows, thin), BF16),
            DMA((3,)), DMA((local_ops,)),
            *dmas((n_blk,), (n_blk,), (n_blk, 2), (n_blk, 2), (n_blk, 2), (n_blk, chips)),
            DMA((n_blk, chips)), pltpu.SemaphoreType.REGULAR((chips,)),
            *dmas((local_ops,), ()),
            *dmas((chips,), (chips,), (chips + 1,), (chips + 1, rest)),
            *dmas((chips + 1, rest), (chips + 1,), (chips,)),
        ],
        compiler_params=pltpu.CompilerParams(
            collective_id=0, has_side_effects=True, vmem_limit_bytes=63 * 2**20
        ),
        name="sigma",
    )(psi, left_blocks, right_ops, block_target, left_partner, block_len)


def solution(mesh):
    return jax.shard_map(
        functools.partial(local, mesh.shape["ops"], mesh.shape["blk"]),
        mesh=mesh,
        in_specs=(
            P("blk", None),
            P("ops", "blk", None, None),
            P(("ops", "blk"), None, None),
            P("ops", None),
            P("ops"),
            P(),
        ),
        out_specs=P("blk", "ops"),
        check_vma=False,
    )
```

```python
import functools

import jax
import jax.numpy as jnp
from jax import lax
from jax.experimental import pallas as pl
from jax.experimental.pallas import tpu as pltpu
from jax.sharding import PartitionSpec as P

MESH = pl.DeviceIdType.MESH
VMEM = pltpu.VMEM
SMEM = pltpu.SMEM
DMA = pltpu.SemaphoreType.DMA
F32 = jnp.float32
BF16 = jnp.bfloat16
scope = jax.named_scope


def across(c, d, n):
    out, bit = 0, 1
    while bit < n:
        out = out + bit * ((c // bit + d // bit) % 2)
        bit *= 2
    return out


def remote(src, dst, send, recv, to):
    return pltpu.make_async_remote_copy(
        src_ref=src, dst_ref=dst, send_sem=send, recv_sem=recv, device_id=to, device_id_type=MESH
    )


def shares(half_rows, chips):
    sizes = [max(half_rows // 2 // chips // 16, 1) * 16] * chips
    return sizes, [sum(sizes[:n]) for n in range(chips)]


def sigma_kernel(
    n_ops, n_blk, psi_hbm, left_hbm, r_hbm, target_ref, pair_ref, len_ref, out_ref,
    own, psi_z, psi_p, left_in, stage, left_v, r_v, img, run, tab_v, tab_s, prev_s, last_s,
    part, recv1, sum1, recv_z, recv_a1, recv_b1, send_a2, recv_a2, send_b2, recv_b2, send3, recv3,
    s_load, s_r, ss_a, sr_a, ss_c, sr_c, ss_f, sr_f, ss_g, sr_g, ss_l, sr_l, ss_z, sr_z, ss_y, above, ss_r, sr_r, ss_t, sr_t,
    ss_1, sr_1, ss_f1, sr_f1, ss_a1, sr_a1, ss_b1, sr_b1, ss_a2, sr_a2, ss_b2, sr_b2, ss_3, sr_3,
):
    g, c = lax.axis_index("ops"), lax.axis_index("blk")
    chips = n_ops // 2
    z, core = g // 2, g % 2
    partner = (z * 2 + (1 - core), c)
    peers = [across(c, d, n_blk) for d in range(n_blk)]
    order = list(range(1, n_blk))

    columns = psi_hbm.shape[1]
    half_rows = psi_hbm.shape[0] // 2
    group, local_blocks, block_rows, _ = left_in.shape
    half_blocks = local_blocks // 2
    local_ops = r_hbm.shape[0]
    thin = out_ref.shape[1]
    wide = 2 * thin
    blocks = target_ref.shape[1]
    pairs = run.shape[0] - 1
    rest = n_blk // 2
    sizes, starts = shares(half_rows, chips)
    climb = sum(sizes)
    straight = half_rows - climb
    ahead = recv_z.shape[3]

    def facing(n):
        return across(z, chips - 1 - n, chips)

    mine = pl.ds(pl.multiple_of(core * half_rows, half_rows), half_rows)
    get_psi = pltpu.make_async_copy(psi_hbm.at[mine], own, s_load.at[0])
    get_left = pltpu.make_async_copy(left_hbm, left_in, s_load.at[1])

    def get_r(r):
        return pltpu.make_async_copy(r_hbm.at[r], r_v.at[0, r], s_r.at[r])

    get_psi.start()

    def by_chip(run_one):
        for chip in range(chips):
            @pl.when(z == chip)
            def _(chip=chip):
                run_one(chip)

    barrier = pltpu.get_barrier_semaphore()
    plane = [partner] + [(z * 2 + k, peers[d]) for d in order for k in range(2)]
    for to in plane:
        pl.semaphore_signal(barrier, inc=1, device_id=to, device_id_type=MESH)
    for e in range(1, chips):
        @pl.when(z + e < chips)
        def _(e=e):
            to = (g + 2 * e, c)
            pl.semaphore_signal(barrier, inc=1, device_id=to, device_id_type=MESH)
    with scope("greet"):
        by_chip(lambda chip: pl.semaphore_wait(barrier, len(plane) + chip))
    for e in range(1, chips):
        @pl.when(z >= e)
        def _(e=e):
            to = (g - 2 * e, c)
            pl.semaphore_signal(above.at[z], inc=1, device_id=to, device_id_type=MESH)

    def rows_of(chip):
        return pl.ds(starts[chip], sizes[chip])

    near_d = [1] + list(range(2, n_blk, 2))
    far_d = list(range(3, n_blk, 2))

    def first(d, chip):
        rows = rows_of(chip)
        return remote(
            own.at[rows], psi_z.at[d, rows], ss_a.at[d], sr_a.at[d], (g, peers[d])
        )

    def plain(d):
        return remote(
            own.at[pl.ds(climb, straight)], psi_p.at[d], ss_c.at[d], sr_c.at[d], (g, peers[d])
        )

    def second(d, way, chip):
        source, to = (d - 1, 1) if way == 0 else (1, d - 1)
        at = pl.ds(starts[chip] + way * (sizes[chip] // 2), sizes[chip] // 2)
        return remote(
            psi_z.at[source, at], psi_z.at[d, at], ss_f.at[d, way], sr_f.at[d, way], (g, peers[to])
        )

    def plain_second(d, way):
        source, to = (d - 1, 1) if way == 0 else (1, d - 1)
        at = pl.ds(way * (straight // 2), straight // 2)
        return remote(
            psi_p.at[source, at], psi_p.at[d, at], ss_g.at[d, way], sr_g.at[d, way], (g, peers[to])
        )

    def along(d, chip, to):
        here = psi_z.at[d, rows_of(chip)]
        return remote(here, here, ss_z.at[d, to], sr_z.at[d, chip], (to * 2 + core, c))

    def passed(d, source, to):
        here = psi_z.at[d, rows_of(source)]
        return remote(here, here, ss_y.at[d, source], sr_z.at[d, source], (to * 2 + core, c))

    def arrived(d, source):
        here = psi_z.at[d, rows_of(source)]
        return remote(here, here, ss_z.at[d, 0], sr_z.at[d, source], partner)

    relays = []
    if chips > 2:
        relays.append((chips - 2, [0], chips - 1))
        relays.append((1, [chips - 1], 0))

    def targets(chip):
        skip = [to for _, sources, to in relays if chip in sources]
        found = [to for to in range(chips) if to != chip and to not in skip]
        return sorted(found, key=lambda to: -abs(to - chip))

    def swap_r(r):
        return remote(r_v.at[0, r], r_v.at[1, r], ss_r.at[r], sr_r.at[r], partner)

    def lefts(d, k):
        which = core if k == 0 else 1 - core
        to = (z * 2 + which, peers[d])
        first_op = pl.multiple_of(peers[d] * local_ops, local_ops)
        return remote(
            stage.at[which, pl.ds(first_op, local_ops)], left_v.at[d, k],
            ss_l.at[d, k], sr_l.at[d, k], to,
        )

    table = remote(tab_v.at[0], tab_v.at[1], ss_t, sr_t, partner)

    def start_plane(chip):
        for d in near_d:
            first(d, chip).start()

    with scope("psi"):
        get_psi.wait()
        get_left.start()
    with scope("start_plane"):
        by_chip(start_plane)
        for d in near_d:
            if straight:
                plain(d).start()
    for r in range(local_ops):
        get_r(r).start()

    tab_v[0] = jnp.zeros_like(tab_v[0])
    for j in range(group):
        tab_v[0, j : j + 1, :blocks] = target_ref[pl.ds(lax.rem(pair_ref[j], group), 1), :]
    table.start()

    with scope("left"):
        get_left.wait()
    lane = lax.broadcasted_iota(jnp.int32, (1, block_rows), 1)

    def put(j, carry):
        owner = lax.rem(pair_ref[j], group)
        for k in range(2):
            for i in range(half_blocks):
                b = k * half_blocks + i
                live = lane < len_ref[c * local_blocks + b]
                block = left_in[owner, b]
                stage[k, j, i] = jnp.where(live, block, jnp.zeros_like(block))
        return carry

    lax.fori_loop(0, group, put, 0)
    def spread_near(chip):
        first(1, chip).wait_recv()
        for f in far_d:
            second(f, 1, chip).start()
        for d in near_d[1:]:
            first(d, chip).wait_recv()
            second(d + 1, 0, chip).start()
        for to in range(chip + 1, chips):
            pl.semaphore_wait(above.at[to], 1)
        for d in near_d:
            for to in targets(chip):
                along(d, chip, to).start()

    with scope("spread_near"):
        by_chip(spread_near)
    for d in near_d:
        lefts(d, 0).start()
    for r in range(local_ops):
        get_r(r).wait()
        swap_r(r).start()
    lefts(0, 1).start()
    left_v[0, 0] = stage[core, pl.ds(c * local_ops, local_ops)]
    run[pairs] = jnp.zeros_like(run[pairs])

    def image(state, first_d, count, at, k):
        rows = state.shape[0] // count

        def one(r, carry):
            out = jnp.dot(state[...], r_v[k, r], preferred_element_type=F32).astype(BF16)
            for d in range(count):
                for j in range(chips):
                    img[j, first_d + d, k, r, at : at + rows] = out[
                        d * rows : (d + 1) * rows, j * wide : (j + 1) * wide
                    ]
            return carry

        lax.fori_loop(0, local_ops, one, 0)

    def image_z(first_d, count, k):
        image(psi_z[first_d : first_d + count].reshape(count * climb, columns), first_d, count, 0, k)

    def image_p(first_d, count, k):
        if straight:
            state = psi_p[first_d : first_d + count].reshape(count * straight, columns)
            image(state, first_d, count, climb, k)

    with scope("image00"):
        image(own, 0, 1, 0, 0)
    table.wait_recv()
    get_table = pltpu.make_async_copy(tab_v, tab_s, s_load.at[2])
    get_table.start()
    get_table.wait()

    def link(p, last):
        i = p % half_blocks
        r = p // half_blocks % local_ops
        k = p // (half_blocks * local_ops) % 2
        d = p // (half_blocks * local_ops * 2)
        q = across(c, d, n_blk) * local_blocks + core * half_blocks + i
        t = tab_s[k, c * local_ops + r, q]
        before = jnp.int32(pairs)
        for b in range(blocks):
            before = jnp.where(t == b, last[b], before)
        prev_s[p] = before
        return tuple(jnp.where(t == b, p, last[b]) for b in range(blocks))

    with scope("link"):
        last = lax.fori_loop(0, pairs, link, (jnp.int32(pairs),) * blocks)
    for b in range(blocks):
        last_s[b] = last[b]

    with scope("plain_near"):
        for d in near_d:
            if straight:
                plain(d).wait_recv()
            for f in far_d:
                if straight and (d == 1 or d == f - 1):
                    plain_second(f, 1 if d == 1 else 0).start()
    for d in near_d:
        lefts(d, 1).start()
    for d in far_d:
        for k in range(2):
            lefts(d, k).start()

    def spread_far(chip):
        for d in far_d:
            for way in range(2):
                second(d, way, chip).wait_recv()
            for to in targets(chip):
                along(d, chip, to).start()

    with scope("spread_far"):
        by_chip(spread_far)

    def pass_on(d):
        for node, sources, to in relays:
            @pl.when(z == node)
            def _(sources=sources, to=to):
                for source in sources:
                    arrived(d, source).wait_recv()
                    passed(d, source, to).start()

    def settle(d):
        for source in range(chips):
            due = z != source
            for node, sources, _ in relays:
                if source in sources:
                    due = jnp.logical_and(due, z != node)

            @pl.when(due)
            def _(source=source):
                arrived(d, source).wait_recv()
    with scope("pass#d=1"):
        pass_on(1)
    with scope("swapr"):
        for r in range(local_ops):
            swap_r(r).wait_recv()
    with scope("image01"):
        image(own, 0, 1, 0, 1)
    tail_d = far_d[-1]
    for d in order[1:]:
        with scope("pass#d=%d" % d):
            pass_on(d)
        if d < tail_d and d % 2 == 0:
            with scope("image_p#d=%d" % d):
                for k in range(2):
                    image_p(d - 1, 2, k)
    with scope("plain_far"):
        for d in far_d if straight else []:
            for way in range(2):
                plain_second(d, way).wait_recv()
    with scope("image_p_far"):
        for k in range(2):
            image_p(tail_d, 1, k)
    for d in range(1, n_blk, 2):
        count = min(2, n_blk - d)
        with scope("settle#d=%d" % d):
            for e in range(count):
                settle(d + e)
        with scope("image_z#d=%d" % d):
            for k in range(2):
                image_z(d, count, k)

    def mix(n):
        j = facing(n)

        def one(p, carry):
            i = p % half_blocks
            r = p // half_blocks % local_ops
            k = p // (half_blocks * local_ops) % 2
            d = p // (half_blocks * local_ops * 2)
            rows = pl.ds(pl.multiple_of(i * block_rows, block_rows), block_rows)
            mixed = jnp.dot(left_v[d, k, r, i], img[j, d, k, r, rows], preferred_element_type=F32)
            run[p] = run[prev_s[p]] + mixed
            return carry

        if n == 0:
            each = pairs // n_blk
            lefts(0, 1).wait_recv()
            for d in range(n_blk):
                for k in range(2 if d else 0):
                    lefts(d, k).wait_recv()
                lax.fori_loop(d * each, (d + 1) * each, one, 0, unroll=min(each, 8))
        else:
            lax.fori_loop(0, pairs, one, 0, unroll=16)

        def emit(d, carry):
            for i in range(local_blocks):
                half, at = i // half_blocks, i % half_blocks
                slot = d % 2 * rest + d // 2 if half == 0 else d
                rows = pl.ds(at * block_rows, block_rows)
                kept = run[last_s[across(c, d, n_blk) * local_blocks + i]].astype(BF16)
                part[n, 0, half, slot, rows] = kept[:, :thin]
                part[n, 1, half, slot, rows] = kept[:, thin:]
            return carry

        lax.fori_loop(0, n_blk, emit, 0)
        swap(n).start()

    def swap(n):
        return remote(part.at[n, 1 - core], recv1.at[n], ss_1.at[n], sr_1.at[n], partner)

    early = pl.ds(0, ahead)
    late = pl.ds(ahead, half_rows - ahead)

    def moved(n):
        return early if n == chips else late

    def chunk(n):
        return min(n, chips - 1)

    def gathers(n):
        offset = chips - 1 - n
        return offset > 1 and offset % 2 == 1

    def crosses(n):
        return 0 < n < chips - 1 and gathers(n - 1)

    final = [n for n in range(chips - 1) if not gathers(n)]

    def toward(n):
        return (facing(chips - 2 if gathers(n) else n) * 2 + core, c)

    def step_z(n):
        return remote(sum1.at[n, :, :, early], recv_z.at[n], ss_f1.at[n], sr_f1.at[n], toward(n))

    def step_a1(n):
        return remote(
            sum1.at[chunk(n), 0, pl.ds(rest, rest), moved(n)], recv_a1.at[chunk(n), :, moved(n)],
            ss_a1.at[n], sr_a1.at[n], (g, peers[1]),
        )

    def step_b1(n, dy):
        return remote(
            sum1.at[chunk(n), 1, pl.ds(2 * dy, 2), moved(n)], recv_b1.at[chunk(n), dy, :, moved(n)],
            ss_b1.at[n, dy], sr_b1.at[n, dy], (g, peers[2 * dy]),
        )

    def step_a2(n, dy):
        return remote(
            send_a2.at[chunk(n), dy, moved(n)], recv_a2.at[chunk(n), dy, moved(n)],
            ss_a2.at[n, dy], sr_a2.at[n, dy], (g, peers[2 * dy]),
        )

    def step_b2(n):
        return remote(
            send_b2.at[chunk(n), moved(n)], recv_b2.at[chunk(n), moved(n)],
            ss_b2.at[n], sr_b2.at[n], (g, peers[1]),
        )

    def last_step(n):
        return remote(
            send3.at[n, :, moved(n)], recv3.at[n, :, moved(n)],
            ss_3.at[n], sr_3.at[n], toward(n),
        )

    def add(n, half, slots):
        m, rows = chunk(n), moved(n)
        both = part[m, core, half, slots, rows].astype(F32) + recv1[m, half, slots, rows].astype(F32)
        if n == chips:
            for e in final:
                both += recv_z[e, half, slots].astype(F32)
        sum1[m, half, slots, rows] = both.astype(BF16)

    def begin(n):
        if n == 0:
            join(n)
        else:
            swap(n).wait_recv()
        for half in range(2):
            both = part[n, core, half, :, early].astype(F32) + recv1[n, half, :, early].astype(F32)
            sum1[n, half, :, early] = both.astype(BF16)
        if not crosses(n):
            step_z(n).start()

    def cross(n):
        step_z(n - 1).wait_recv()
        for half in range(2):
            both = sum1[n, half, :, early].astype(F32) + recv_z[n - 1, half].astype(F32)
            sum1[n, half, :, early] = both.astype(BF16)
        step_z(n).start()

    def join(n):
        if n in (0, chips - 1):
            swap(n).wait_recv()
        if n == chips:
            for e in final:
                step_z(e).wait_recv()
        add(n, 0, pl.ds(rest, rest))
        step_a1(n).start()
        add(n, 1, pl.ds(2, n_blk - 2))
        for dy in range(1, rest):
            step_b1(n, dy).start()
        add(n, 0, pl.ds(0, rest))
        add(n, 1, pl.ds(0, 2))

    def middle(n):
        m, rows = chunk(n), moved(n)
        step_a1(n).wait_recv()
        for dy in range(1, rest):
            both = sum1[m, 0, dy, rows].astype(F32) + recv_a1[m, dy, rows].astype(F32)
            send_a2[m, dy, rows] = both.astype(BF16)
            step_a2(n, dy).start()
        both = sum1[m, 1, 1, rows].astype(F32)
        for dy in range(1, rest):
            step_b1(n, dy).wait_recv()
            both += recv_b1[m, dy, 1, rows].astype(F32)
        send_b2[m, rows] = both.astype(BF16)
        step_b2(n).start()

    row = lax.broadcasted_iota(jnp.int32, (block_rows, 1), 0)

    def put_out(half, value, first_row):
        size = value.shape[0]
        for i in range(half_blocks):
            low = max(first_row, i * block_rows)
            high = min(first_row + size, (i + 1) * block_rows)
            if low < high:
                kept = value[low - first_row : high - first_row]
                live = row[low - i * block_rows : high - i * block_rows] < len_ref[
                    c * local_blocks + half * half_blocks + i
                ]
                kept = jnp.where(live, kept, jnp.zeros_like(kept)).astype(out_ref.dtype)
                out_ref[half * half_rows + low : half * half_rows + high] = kept

    def finish(n):
        m, rows = chunk(n), moved(n)
        a = sum1[m, 0, 0, rows].astype(F32) + recv_a1[m, 0, rows].astype(F32)
        b = sum1[m, 1, 0, rows].astype(F32)
        for dy in range(1, rest):
            step_a2(n, dy).wait_recv()
            a += recv_a2[m, dy, rows].astype(F32)
            b += recv_b1[m, dy, 0, rows].astype(F32)
        step_b2(n).wait_recv()
        b += recv_b2[m, rows].astype(F32)
        if crosses(n):
            last_step(n - 1).wait_recv()
            a += recv3[n - 1, 0, rows].astype(F32)
            b += recv3[n - 1, 1, rows].astype(F32)
        if n < chips - 1:
            send3[n, 0, rows] = a.astype(BF16)
            send3[n, 1, rows] = b.astype(BF16)
            last_step(n).start()
            return
        if n == chips - 1:
            for e in final:
                last_step(e).wait_recv()
                a += recv3[e, 0, rows].astype(F32)
                b += recv3[e, 1, rows].astype(F32)
        put_out(0, a, 0 if n == chips else ahead)
        put_out(1, b, 0 if n == chips else ahead)

    def drain_gather():
        table.wait_send()
        lefts(0, 1).wait_send()
        for r in range(local_ops):
            swap_r(r).wait_send()

        def drain(chip):
            for d in near_d:
                first(d, chip).wait_send()
            for d in far_d:
                for way in range(2):
                    second(d, way, chip).wait_send()
            for d in order:
                for to in targets(chip):
                    along(d, chip, to).wait_send()

        by_chip(drain)
        for d in order:
            for node, sources, to in relays:
                @pl.when(z == node)
                def _(d=d, sources=sources, to=to):
                    for source in sources:
                        passed(d, source, to).wait_send()
            for k in range(2):
                lefts(d, k).wait_send()
        for d in near_d if straight else []:
            plain(d).wait_send()
        for d in far_d if straight else []:
            for way in range(2):
                plain_second(d, way).wait_send()

    def drain_steps(n):
        step_a1(n).wait_send()
        step_b2(n).wait_send()
        for dy in range(1, rest):
            step_b1(n, dy).wait_send()
            step_a2(n, dy).wait_send()

    def perform(stage_of, n):
        with scope("%s#n=%d" % (stage_of.__name__, n)):
            stage_of(n)

    perform(mix, 0)
    for n in range(1, chips):
        perform(mix, n)
        perform(begin, n - 1)
        if n == 2:
            perform(join, 1)
    for n in range(chips):
        if crosses(n):
            perform(cross, n)
    for n in range(chips):
        if n == 1:
            drain_gather()
        perform(middle, n)
        if n and n != chips - 2:
            perform(finish, n - 1)
        if n == chips - 2:
            perform(finish, n - 1)
            perform(join, chips)
        if 2 <= n + 2 < chips:
            perform(join, n + 2)
    for n in range(chips):
        swap(n).wait_send()
    for n in range(chips - 1):
        step_z(n).wait_send()
    for n in range(chips - 2):
        drain_steps(n)
    perform(middle, chips)
    perform(finish, chips)
    perform(finish, chips - 1)

    for n in range(chips - 2, chips + 1):
        drain_steps(n)
    for n in range(chips - 1):
        last_step(n).wait_send()


def local(n_ops, n_blk, psi, left_blocks, right_ops, block_target, left_partner, block_len):
    group, local_blocks, block_rows, _ = left_blocks.shape
    my_rows, columns = psi.shape
    local_ops = right_ops.shape[0]
    blocks = block_target.shape[1]
    chips = n_ops // 2
    thin = columns // n_ops
    wide = 2 * thin
    half_rows, half_blocks = my_rows // 2, local_blocks // 2
    rest = n_blk // 2
    pairs = n_blk * 2 * local_ops * half_blocks
    in_vmem = pl.BlockSpec(memory_space=pltpu.VMEM)
    in_smem = pl.BlockSpec(memory_space=pltpu.SMEM)
    in_hbm = pl.BlockSpec(memory_space=pl.ANY)

    def dmas(*shapes):
        return [DMA(shape) for shape in shapes for _ in range(2)]

    return pl.pallas_call(
        functools.partial(sigma_kernel, n_ops, n_blk),
        out_shape=pltpu.VMEM((my_rows, thin), BF16),
        in_specs=[in_hbm, in_hbm, in_hbm, in_vmem, in_smem, in_smem],
        out_specs=in_vmem,
        scratch_shapes=[
            VMEM((half_rows, columns), BF16),
            VMEM((n_blk, sum(shares(half_rows, chips)[0]), columns), BF16),
            VMEM((n_blk, max(half_rows - sum(shares(half_rows, chips)[0]), 16), columns), BF16),
            VMEM(left_blocks.shape, BF16),
            VMEM((2, group, half_blocks, block_rows, block_rows), BF16),
            VMEM((n_blk, 2, local_ops, half_blocks, block_rows, block_rows), BF16),
            VMEM((2, local_ops, columns, columns), BF16),
            VMEM((chips, n_blk, 2, local_ops, half_rows, wide), BF16),
            VMEM((pairs + 1, block_rows, wide), F32),
            VMEM((2, group, 128), jnp.int32),
            SMEM((2, group, 128), jnp.int32),
            SMEM((pairs,), jnp.int32),
            SMEM((blocks,), jnp.int32),
            VMEM((chips, 2, 2, n_blk, half_rows, thin), BF16),
            VMEM((chips, 2, n_blk, half_rows, thin), BF16),
            VMEM((chips, 2, n_blk, half_rows, thin), BF16),
            VMEM((max(chips - 1, 1), 2, n_blk, max(half_rows * 7 // 32 // 8, 1) * 8, thin), BF16),
            VMEM((chips, rest, half_rows, thin), BF16),
            VMEM((chips, rest, 2, half_rows, thin), BF16),
            VMEM((chips, rest, half_rows, thin), BF16),
            VMEM((chips, rest, half_rows, thin), BF16),
            VMEM((chips, half_rows, thin), BF16),
            VMEM((chips, half_rows, thin), BF16),
            VMEM((chips, 2, half_rows, thin), BF16),
            VMEM((chips, 2, half_rows, thin), BF16),
            DMA((3,)), DMA((local_ops,)),
            *dmas((n_blk,), (n_blk,), (n_blk, 2), (n_blk, 2), (n_blk, 2), (n_blk, chips)),
            DMA((n_blk, chips)), pltpu.SemaphoreType.REGULAR((chips,)),
            *dmas((local_ops,), ()),
            *dmas((chips,), (chips,), (chips + 1,), (chips + 1, rest)),
            *dmas((chips + 1, rest), (chips + 1,), (chips,)),
        ],
        compiler_params=pltpu.CompilerParams(
            collective_id=0, has_side_effects=True, vmem_limit_bytes=63 * 2**20
        ),
        name="sigma",
    )(psi, left_blocks, right_ops, block_target, left_partner, block_len)


def solution(mesh):
    return jax.shard_map(
        functools.partial(local, mesh.shape["ops"], mesh.shape["blk"]),
        mesh=mesh,
        in_specs=(
            P("blk", None),
            P("ops", "blk", None, None),
            P(("ops", "blk"), None, None),
            P("ops", None),
            P("ops"),
            P(),
        ),
        out_specs=P("blk", "ops"),
        check_vma=False,
    )
```
